32 devices in a mesh: blk: 8 (over z, x), ga: 4 (over y, core).
Axes of the slice: x: 2, y: 2, z: 4, core: 2. Of those that a mesh axis runs over, the one named last changes fastest.
Arguments:
- pair_val: bfloat16 [16, 16, 16, 2048], P('blk', None, None, 'ga'), may hold values from -0.125 to 0.125
- pair_con: bfloat16 [16, 16, 16, 2048], P('blk', None, None, 'ga'), may hold values from -6 to 6
- screened: bfloat16 [16, 2048, 2048], P('blk', None, 'ga'), may hold values from -0.125 to 0.125
- amplitude: bfloat16 [16, 16], P('blk'), may hold values from -6 to 6
- qmap: int32 [16, 16], P('blk'), may hold values from 0 to 15, as said below
Outputs:
- kernel_x: float32 [16, 16], P('blk')
The draws below stay inside these ranges and needn't reach their ends.
Inputs may be any that keep to these rules, and one draw needn't show every extreme that they name: qmap[k, k'] is the label of the difference k - k' (periodic) on a grid of 8 by 2 points, with the points and the differences labelled at random; every row and every column holds each label once.
All inputs are finite; a program needn't handle non-finite values.
Results may differ from the reference program's by a relative error of at most 0.004.
Values may be sent and summed in bfloat16 or wider, within the bound.
A program may use at most 64 MiB of HBM per device.

```python
import jax
import jax.numpy as jnp
from jax import lax

NV = 4
NC = 4
NG = 2048
GRID_X = 8
NK = 16


def draw_qmap(key, part):
    point_order = jax.random.permutation(jax.random.fold_in(key, 11), NK)
    label_order = jax.random.permutation(jax.random.fold_in(key, 23), NK)
    rows_y = NK // GRID_X
    coord_x = point_order % GRID_X
    coord_y = point_order // GRID_X
    diff_x = (coord_x[:, None] - coord_x[None, :]) % GRID_X
    diff_y = (coord_y[:, None] - coord_y[None, :]) % rows_y
    return label_order[diff_y * GRID_X + diff_x].astype(jnp.int32)


def block_scale(own_key, shape, shards, smallest, high):
    factor_of, own = 1.0, jax.random.fold_in(own_key, 6)
    for dim, shards_of in shards:
        steps = jnp.exp(jax.random.uniform(jax.random.fold_in(own, dim), (shards_of,), jnp.float32, smallest / len(shards), high / len(shards)))
        factor_of = factor_of * jnp.repeat(steps, shape[dim] // shards_of).reshape([-1 if axis == dim else 1 for axis in range(len(shape))])
    return factor_of


def bell_draw(stream_key, shape, width, reach, pieces=(), held_as=jnp.bfloat16):
    values = width * jax.random.normal(stream_key, shape, jnp.float32)
    if pieces:
        values = values * block_scale(stream_key, shape, pieces, -0.22, 0.18)
    return jnp.clip(values, -reach, reach).astype(held_as)


def setup_inputs(seed: int = 0) -> dict:
    key_list = jax.random.split(jax.random.key(seed), 6)
    return {
        "pair_val": bell_draw(key_list[0], (NK, NK, NV * NV, NG), NG ** -0.5, 0.125, ((0, 8), (3, 4))),
        "pair_con": bell_draw(key_list[1], (NK, NK, NC * NC, NG), 1.0, 6.0, ((0, 8), (3, 4))),
        "screened": bell_draw(key_list[2], (NK, NG, NG), NG ** -0.5, 0.125, ((0, 8), (2, 4))),
        "amplitude": bell_draw(key_list[3], (NK, NV * NC), 1.0, 6.0, ((0, 8),)),
        "qmap": draw_qmap(jax.random.fold_in(key_list[5], 71), 0),
    }


def inverse_rows(qmap):
    total = qmap.shape[1]
    labels = jnp.arange(total, dtype=jnp.int32)
    hits = (qmap[:, :, None] == labels[None, None, :]).astype(jnp.int32)
    return jnp.sum(hits * labels[None, :, None], axis=1).astype(jnp.int32)


def reference(pair_val, pair_con, screened, amplitude, qmap):
    total = qmap.shape[0]
    partner = inverse_rows(qmap)
    rows = jnp.arange(total, dtype=jnp.int32)

    def per_label(label):
        chosen = lax.dynamic_index_in_dim(partner, label, 1, keepdims=False).astype(jnp.int32)
        values = pair_val[rows, chosen].astype(jnp.float32).reshape(total, NV, NV, NG)
        cons = pair_con[rows, chosen]
        amps = amplitude[chosen].astype(jnp.float32).reshape(total, NV, NC)
        zeta = jnp.einsum('navg,nvc->nacg', values, amps).astype(jnp.bfloat16)
        zeta = lax.optimization_barrier(zeta).astype(jnp.float32)
        weights = lax.dynamic_index_in_dim(screened, label, 0, keepdims=False)
        unit = jnp.dot(cons.reshape(total * NC * NC, NG), weights, preferred_element_type=jnp.float32).astype(jnp.bfloat16)
        unit = lax.optimization_barrier(unit).astype(jnp.float32).reshape(total, NC, NC, NG)
        return jnp.einsum('ncyg,nayg->nac', unit, zeta).reshape(total, NV * NC)

    parts = lax.map(per_label, rows)
    return jnp.sum(parts, 0) / total
```

```python
import functools

import jax
import jax.numpy as jnp
from jax import lax
from jax.experimental import pallas as pl
from jax.experimental.pallas import tpu as pltpu
from jax.sharding import PartitionSpec as P

NV = 4
NC = 4
ROWS = 16
TILE = 256
MESH = pl.DeviceIdType.MESH
F32 = jnp.float32
BF16 = jnp.bfloat16


def iota(shape, dim):
    return lax.broadcasted_iota(jnp.int32, shape, dim)


def one_hot(mask):
    return jnp.where(mask, 1.0, 0.0).astype(F32)


def kernel(
    blks, gas, val_hbm, con_hbm, w_hbm, amp_hbm, q_hbm, out_ref,
    q_in, amp_in, val_in, con_in, w_in, con_send, zeta_send, con_all, zeta_all, amp_all, amp_rows, unit, contrib, fin,
    load_sem, amp_ssem, amp_rsem, con_ssem, con_rsem, zeta_ssem, zeta_rsem,
    row_ssem, row_rsem, core_ssem, core_rsem, fin_ssem, fin_rsem,
):
    me, ga = lax.axis_index("blk"), lax.axis_index("ga")
    local_k, total = q_in.shape
    labels, width = w_in.shape[0], w_in.shape[2]
    wide = total * ROWS
    lane = me * gas + ga
    devices = blks * gas
    rings = gas // 2
    other = ga + 1 - 2 * (ga % 2)

    barrier = pltpu.get_barrier_semaphore()
    for step in range(1, blks):
        pl.semaphore_signal(barrier, inc=1, device_id=((me + step) % blks, ga), device_id_type=MESH)
    pl.semaphore_signal(barrier, inc=1, device_id=(me, other), device_id_type=MESH)
    for hop in range(1, rings):
        pl.semaphore_signal(barrier, inc=1, device_id=(me, (ga + 2 * hop) % gas), device_id_type=MESH)

    q_load = pltpu.make_async_copy(q_hbm, q_in, load_sem.at[0])
    amp_load = pltpu.make_async_copy(amp_hbm, amp_in, load_sem.at[1])
    val_load = pltpu.make_async_copy(val_hbm, val_in, load_sem.at[2])
    w_load = pltpu.make_async_copy(w_hbm, w_in, load_sem.at[3])
    con_loads = [pltpu.make_async_copy(con_hbm.at[k], con_in.at[k], load_sem.at[4 + k]) for k in range(local_k)]
    for load in [q_load, *con_loads, amp_load, val_load, w_load]:
        load.start()

    line = blks // 2
    z, x = me // 2, me % 2

    def both(*steps):
        return [(sign * far, turn) for far in steps for turn in (1, 0) for sign in (1, -1)]

    far_first = both(*range(line - 1, 1, -1))
    con_order = both(1) + [(0, 1)] + far_first
    zeta_order = [(0, 1)] + far_first + both(1)

    def to_blk(shift):
        return (z + shift[0]) * 2 + (x + shift[1]) % 2

    def from_blk(shift):
        return (z - shift[0]) * 2 + (x + shift[1]) % 2

    def sent(chosen, action):
        for shift in chosen:
            pl.when((z + shift[0] >= 0) & (z + shift[0] < line))(functools.partial(action, shift))

    def received(chosen, action):
        for shift in chosen:
            pl.when((z - shift[0] >= 0) & (z - shift[0] < line))(functools.partial(action, shift))

    def blk_copy(src, dst, ssem, rsem, to):
        return pltpu.make_async_remote_copy(
            src_ref=src, dst_ref=dst, send_sem=ssem.at[to], recv_sem=rsem.at[me],
            device_id=(to, ga), device_id_type=MESH)

    def amp_copy(shift):
        return blk_copy(amp_in, amp_all.at[me], amp_ssem, amp_rsem, to_blk(shift))

    def con_copy(shift):
        to = to_blk(shift)
        return blk_copy(con_send.at[to], con_all.at[ga, me], con_ssem, con_rsem, to)

    def zeta_copy(shift):
        to = to_blk(shift)
        return blk_copy(zeta_send.at[to], zeta_all.at[me], zeta_ssem, zeta_rsem, to)

    def arrival(ref, ssem, rsem, owner):
        return pltpu.make_async_remote_copy(
            src_ref=ref, dst_ref=ref, send_sem=ssem.at[owner], recv_sem=rsem.at[owner],
            device_id=(owner, ga), device_id_type=MESH)

    def row_copy(hop, owner):
        return pltpu.make_async_remote_copy(
            src_ref=con_all.at[ga, owner], dst_ref=con_all.at[ga, owner],
            send_sem=row_ssem.at[hop, owner], recv_sem=row_rsem.at[hop, owner],
            device_id=(me, (ga + 2 * hop) % gas), device_id_type=MESH)

    def core_copy(hop, owner):
        part = (ga + gas - 2 * hop) % gas
        return pltpu.make_async_remote_copy(
            src_ref=con_all.at[part, owner], dst_ref=con_all.at[part, owner],
            send_sem=core_ssem.at[hop, owner], recv_sem=core_rsem.at[hop, owner],
            device_id=(me, other), device_id_type=MESH)

    def hand_on(owner):
        for hop in range(1, rings):
            row_copy(hop, owner).start()
        core_copy(0, owner).start()

    def across(owner):
        for hop in range(1, rings):
            row_copy(hop, owner).wait_recv()
            core_copy(hop, owner).start()

    def relay(shift):
        owner = from_blk(shift)
        arrival(con_all.at[ga, owner], con_ssem, con_rsem, owner).wait_recv()
        hand_on(owner)

    spread = one_hot(iota((total, wide), 1) >> 4 == iota((total, wide), 0)).astype(BF16)
    row, col = iota((TILE, wide), 0), iota((TILE, wide), 1)
    same_pair = (row & 15) == (col & 15)
    same_band = ((row >> 2) & 3) == ((col >> 2) & 3)
    chunk_labels = TILE // ROWS
    chunk_blks = chunk_labels // labels

    def stored(ref, k, chunk, value):
        blocks = value.astype(BF16).reshape(chunk_blks, labels, ROWS, width)
        ref[pl.ds(chunk * chunk_blks, chunk_blks), :, pl.ds(k * ROWS, ROWS), :] = blocks

    q_load.wait()
    labels_at = jnp.dot(q_in[...].astype(F32).astype(BF16), spread, preferred_element_type=F32).astype(jnp.int32)
    hits = {}
    for k in range(local_k):
        for chunk in range(wide // TILE):
            hits[k, chunk] = labels_at[k : k + 1, :] == (row >> 4) + chunk * chunk_labels
    for k in range(local_k):
        con_loads[k].wait()
        con_k = con_in[k].reshape(wide, width)
        for chunk in range(wide // TILE):
            pick = one_hot(hits[k, chunk] & same_pair).astype(BF16)
            stored(con_send, k, chunk, jnp.dot(pick, con_k, preferred_element_type=F32))
    amp_load.wait()

    pl.semaphore_wait(barrier, blks - 1 + rings)
    sent(con_order, lambda shift: amp_copy(shift).start())
    sent(con_order, lambda shift: con_copy(shift).start())
    con_all[ga, me] = con_send[me]
    amp_all[me] = amp_in[...]
    hand_on(me)

    received(
        con_order,
        lambda shift: arrival(amp_all.at[from_blk(shift)], amp_ssem, amp_rsem, from_blk(shift)).wait_recv())
    for blk in range(blks):
        amp_rows[pl.ds(blk * local_k, local_k), :] = amp_all[blk].astype(F32)
    amps = lax.dot_general(
        amp_rows[...].astype(BF16), spread, (((0,), (0,)), ((), ())), preferred_element_type=F32)
    pair, at = iota((NV * NC, wide), 0), iota((NV * NC, wide), 1)
    amps = jnp.where((pair >> 2) == (at & 3), amps, 0.0).astype(BF16)
    lines, pairs = iota((TILE, NV * NC), 0), iota((TILE, NV * NC), 1)
    amps = jnp.dot(one_hot((lines & 3) == (pairs & 3)).astype(BF16), amps, preferred_element_type=F32)
    amps = jnp.where(same_band, amps, 0.0)
    val_load.wait()
    for k in range(local_k):
        val_k = val_in[k].reshape(wide, width)
        for chunk in range(wide // TILE):
            mix = jnp.where(hits[k, chunk], amps, 0.0).astype(BF16)
            stored(zeta_send, k, chunk, jnp.dot(mix, val_k, preferred_element_type=F32))
    sent(zeta_order, lambda shift: zeta_copy(shift).start())
    zeta_all[me] = zeta_send[me]

    received(con_order, relay)
    across(me)
    received(con_order, lambda shift: across(from_blk(shift)))

    def gathered(owner):
        for hop in range(rings):
            core_copy(hop, owner).wait_recv()

    w_load.wait()
    for owner in range(blks):
        gathered(owner)

    block = local_k * ROWS
    group = TILE // block
    for part in range(blks // group):
        for label in range(labels):
            summed = None
            for quarter in range(gas):
                cons = con_all[quarter, pl.ds(part * group, group), label].reshape(TILE, width)
                term = jnp.dot(cons, w_in[label, pl.ds(quarter * width, width), :], preferred_element_type=F32)
                summed = term if summed is None else summed + term
            unit[pl.ds(part * group, group), label] = summed.astype(BF16).reshape(group, block, width)

    plane = 2 * block
    r, s = iota((plane, plane), 0), iota((plane, plane), 1)
    kept = ((r >> 4) == (s >> 4)) & ((r & 3) == (s & 3))
    c_at, w_of = iota((ROWS, 128), 0), iota((ROWS, 128), 1)
    by_c = one_hot((c_at >> 2) == (w_of & 3))
    s_at, w_at = iota((plane, 128), 0), iota((plane, 128), 1)
    by_v = (((s_at >> 2) & 3) == ((w_at >> 2) & 3)) & ((s_at >> 4) % local_k == (w_at >> 4))

    def fin_copy(to):
        return pltpu.make_async_remote_copy(
            src_ref=contrib.at[to // gas], dst_ref=fin.at[lane],
            send_sem=fin_ssem.at[to], recv_sem=fin_rsem.at[lane],
            device_id=(to // gas, to % gas), device_id_type=MESH)

    def finish(at):
        first = 2 * at
        for turn in range(2):
            owner = first + turn

            @pl.when(owner != me)
            def _():
                arrival(zeta_all.at[owner], zeta_ssem, zeta_rsem, owner).wait_recv()
        cross = None
        for label in range(labels):
            units = unit[pl.ds(first, 2), label].reshape(plane, width)
            zetas = zeta_all[pl.ds(first, 2), label].reshape(plane, width)
            term = lax.dot_general(units, zetas, (((1,), (1,)), ((), ())), preferred_element_type=F32)
            cross = term if cross is None else cross + term
        folded = jnp.sum(jnp.where(kept, cross, 0.0).reshape(plane // ROWS, ROWS, plane), axis=0)
        spread_c = lax.dot_general(
            folded, by_c, (((0,), (0,)), ((), ())), precision=lax.Precision.HIGHEST, preferred_element_type=F32)
        spread_c = jnp.where(by_v, spread_c, 0.0)
        contrib[pl.ds(first, 2)] = jnp.sum(spread_c.reshape(2, block, 128), axis=1, keepdims=True)
        for turn in range(2):
            for part in range(gas):
                to = (first + turn) * gas + part

                @pl.when(to != lane)
                def _():
                    fin_copy(to).start()

                @pl.when(to == lane)
                def _():
                    fin[lane] = contrib[me]

    low = z < line // 2
    near_end = jnp.where(low, z, line - 1 - z)
    finish(z)
    for step in range(line - 1):
        alone = line - 1 - 2 * near_end
        turn = step - alone
        away = near_end - turn // 2
        place = jnp.where(step < alone, line - 1 - step, near_end + away * (1 - 2 * (turn % 2)))
        finish(jnp.where(low, place, line - 1 - place))

    sent(con_order, lambda shift: amp_copy(shift).wait_send())
    sent(con_order, lambda shift: con_copy(shift).wait_send())
    sent(con_order, lambda shift: zeta_copy(shift).wait_send())
    for owner in range(blks):
        for hop in range(1, rings):
            row_copy(hop, owner).wait_send()
        for hop in range(rings):
            core_copy(hop, owner).wait_send()

    def every(i, carry):
        to = (lane + i) % devices
        fin_copy(to).wait_send()
        pltpu.make_async_remote_copy(
            src_ref=fin.at[to], dst_ref=fin.at[to], send_sem=fin_ssem.at[to], recv_sem=fin_rsem.at[to],
            device_id=(to // gas, to % gas), device_id_type=MESH).wait_recv()
        return carry

    lax.fori_loop(1, devices, every, 0)
    total_row = jnp.sum(fin[...], axis=0) / total
    for k in range(local_k):
        out_ref[k : k + 1, :] = total_row[:, k * ROWS : (k + 1) * ROWS]


def body(pair_val, pair_con, screened, amplitude, qmap, *, blks, gas):
    local_k, total, _, width = pair_val.shape
    labels, depth, _ = screened.shape
    devices = blks * gas
    dma = pltpu.SemaphoreType.DMA
    anywhere = pl.BlockSpec(memory_space=pl.ANY)
    vmem = pl.BlockSpec(memory_space=pltpu.VMEM)
    block = (labels, local_k * ROWS, width)
    return pl.pallas_call(
        functools.partial(kernel, blks, gas),
        out_shape=pltpu.VMEM((local_k, NV * NC), F32),
        in_specs=[anywhere] * 5,
        out_specs=vmem,
        scratch_shapes=[
            pltpu.VMEM(qmap.shape, jnp.int32),
            pltpu.VMEM(amplitude.shape, BF16),
            pltpu.VMEM(pair_val.shape, BF16),
            pltpu.VMEM(pair_con.shape, BF16),
            pltpu.VMEM(screened.shape, BF16),
            pltpu.VMEM((blks,) + block, BF16),
            pltpu.VMEM((blks,) + block, BF16),
            pltpu.VMEM((gas, blks) + block, BF16),
            pltpu.VMEM((blks,) + block, BF16),
            pltpu.VMEM((blks,) + amplitude.shape, BF16),
            pltpu.VMEM((total, NV * NC), F32),
            pltpu.VMEM((blks,) + block, BF16),
            pltpu.VMEM((blks, 1, 128), F32),
            pltpu.VMEM((devices, 1, 128), F32),
            dma((4 + local_k,)),
            *[dma((blks,))] * 6,
            *[dma((gas // 2, blks))] * 4,
            dma((devices,)), dma((devices,)),
        ],
        compiler_params=pltpu.CompilerParams(
            collective_id=0, has_side_effects=True, vmem_limit_bytes=60 * 1024 * 1024),
    )(pair_val, pair_con, screened, amplitude, qmap)


def solution(mesh):
    placed = (
        P("blk", None, None, "ga"),
        P("blk", None, None, "ga"),
        P("blk", None, "ga"),
        P("blk", None),
        P("blk", None),
    )
    sizes = {"blks": mesh.shape["blk"], "gas": mesh.shape["ga"]}
    return jax.shard_map(
        functools.partial(body, **sizes), mesh=mesh, in_specs=placed, out_specs=P("blk", None), check_vma=False
    )
```

```python
import functools

import jax
import jax.numpy as jnp
from jax import lax
from jax.experimental import pallas as pl
from jax.experimental.pallas import tpu as pltpu
from jax.sharding import PartitionSpec as P

NV = 4
NC = 4
ROWS = 16
TILE = 256
LANES = 128
MESH = pl.DeviceIdType.MESH
F32 = jnp.float32
BF16 = jnp.bfloat16


def iota(shape, dim):
    return lax.broadcasted_iota(jnp.int32, shape, dim)


def one_hot(mask):
    return jnp.where(mask, 1.0, 0.0).astype(F32)


def kernel(
    blks, gas, val_hbm, con_hbm, w_hbm, amp_hbm, q_hbm, out_ref,
    q_in, amp_in, val_in, con_in, w_in, con_send, zeta_send, con_all, zeta_all, amp_all, amp_rows, unit, contrib, fin,
    load_sem, send_sem, amp_rsem, con_rsem, zeta_rsem, row_rsem, core_rsem, fin_rsem,
):
    me, ga = lax.axis_index("blk"), lax.axis_index("ga")
    local_k, total = q_in.shape
    labels, width = w_in.shape[0], w_in.shape[2]
    wide = total * ROWS
    lane = me * gas + ga
    devices = blks * gas
    rings = gas // 2
    other = ga + 1 - 2 * (ga % 2)

    barrier = pltpu.get_barrier_semaphore()
    for step in range(1, blks):
        pl.semaphore_signal(barrier, inc=1, device_id=((me + step) % blks, ga), device_id_type=MESH)
    pl.semaphore_signal(barrier, inc=1, device_id=(me, other), device_id_type=MESH)
    for hop in range(1, rings):
        pl.semaphore_signal(barrier, inc=1, device_id=(me, (ga + 2 * hop) % gas), device_id_type=MESH)

    q_load = pltpu.make_async_copy(q_hbm, q_in, load_sem.at[0])
    amp_load = pltpu.make_async_copy(amp_hbm, amp_in, load_sem.at[1])
    val_load = pltpu.make_async_copy(val_hbm, val_in, load_sem.at[2])
    w_load = pltpu.make_async_copy(w_hbm, w_in, load_sem.at[3])
    con_loads = [pltpu.make_async_copy(con_hbm.at[k], con_in.at[k], load_sem.at[4 + k]) for k in range(local_k)]
    for load in [q_load, *con_loads, amp_load]:
        load.start()

    line = blks // 2
    z, x = me // 2, me % 2

    def both(*steps):
        return [(sign * far, turn) for far in steps for turn in (1, 0) for sign in (1, -1)]

    far_first = both(*range(line - 1, 1, -1))
    near = both(1) + [(0, 1)]
    con_order = near + far_first
    zeta_order = [(0, 1)] + far_first + both(1)

    def to_blk(shift):
        return (z + shift[0]) * 2 + (x + shift[1]) % 2

    def from_blk(shift):
        return (z - shift[0]) * 2 + (x + shift[1]) % 2

    def sent(chosen, action):
        for shift in chosen:
            pl.when((z + shift[0] >= 0) & (z + shift[0] < line))(functools.partial(action, shift))

    def received(chosen, action):
        for shift in chosen:
            pl.when((z - shift[0] >= 0) & (z - shift[0] < line))(functools.partial(action, shift))

    def blk_copy(src, dst, ssem, rsem, to):
        return pltpu.make_async_remote_copy(
            src_ref=src, dst_ref=dst, send_sem=ssem, recv_sem=rsem, device_id=(to, ga), device_id_type=MESH)

    def amp_copy(shift):
        return blk_copy(amp_in, amp_all.at[me], send_sem.at[0], amp_rsem, to_blk(shift))

    def con_copy(shift):
        to = to_blk(shift)
        return blk_copy(con_send.at[to], con_all.at[ga, me], send_sem.at[1], con_rsem.at[me], to)

    def zeta_copy(shift):
        to = to_blk(shift)
        return blk_copy(zeta_send.at[to], zeta_all.at[me], send_sem.at[2], zeta_rsem.at[me], to)

    def awaited(ref, sem):
        return pltpu.make_async_remote_copy(
            src_ref=ref, dst_ref=ref, send_sem=sem, recv_sem=sem, device_id=(me, other), device_id_type=MESH)

    def row_copy(hop, owner):
        return pltpu.make_async_remote_copy(
            src_ref=con_all.at[ga, owner], dst_ref=con_all.at[ga, owner],
            send_sem=send_sem.at[3], recv_sem=row_rsem.at[hop - 1, owner],
            device_id=(me, (ga + 2 * hop) % gas), device_id_type=MESH)

    def core_copy(hop, owner):
        part = (ga + gas - 2 * hop) % gas
        return pltpu.make_async_remote_copy(
            src_ref=con_all.at[part, owner], dst_ref=con_all.at[part, owner],
            send_sem=send_sem.at[4], recv_sem=core_rsem.at[owner // (blks // 2)],
            device_id=(me, other), device_id_type=MESH)

    def hand_on(owner):
        for hop in range(1, rings):
            row_copy(hop, owner).start()
        core_copy(0, owner).start()

    def across(owner):
        for hop in range(1, rings):
            row_copy(hop, owner).wait_recv()
            core_copy(hop, owner).start()

    def relay(shift):
        owner = from_blk(shift)
        awaited(con_all.at[ga, owner], con_rsem.at[owner]).wait_recv()
        hand_on(owner)

    spread = one_hot(iota((total, wide), 1) >> 4 == iota((total, wide), 0)).astype(BF16)
    row, col = iota((TILE, wide), 0), iota((TILE, wide), 1)
    same_pair = (row & 15) == (col & 15)
    same_band = ((row >> 2) & 3) == ((col >> 2) & 3)
    chunk_labels = TILE // ROWS
    chunk_blks = chunk_labels // labels

    def stored(ref, k, chunk, value):
        blocks = value.astype(BF16).reshape(chunk_blks, labels, ROWS, width)
        ref[pl.ds(chunk * chunk_blks, chunk_blks), :, pl.ds(k * ROWS, ROWS), :] = blocks

    q_load.wait()
    labels_at = jnp.dot(q_in[...].astype(F32).astype(BF16), spread, preferred_element_type=F32).astype(jnp.int32)
    hits = {}
    for k in range(local_k):
        for chunk in range(wide // TILE):
            hits[k, chunk] = labels_at[k : k + 1, :] == (row >> 4) + chunk * chunk_labels
    for k in range(local_k):
        con_loads[k].wait()
        con_k = con_in[k].reshape(wide, width)
        for chunk in range(wide // TILE):
            pick = one_hot(hits[k, chunk] & same_pair).astype(BF16)
            stored(con_send, k, chunk, jnp.dot(pick, con_k, preferred_element_type=F32))
    amp_load.wait()
    val_load.start()
    w_load.start()

    pl.semaphore_wait(barrier, blks - 1 + rings)
    sent(con_order, lambda shift: amp_copy(shift).start())
    sent(con_order, lambda shift: con_copy(shift).start())
    con_all[ga, me] = con_send[me]
    amp_all[me] = amp_in[...]
    hand_on(me)

    received(near, relay)

    awaited(amp_all.at[pl.ds(0, blks - 1)], amp_rsem).wait_recv()
    for blk in range(blks):
        amp_rows[pl.ds(blk * local_k, local_k), :] = amp_all[blk].astype(F32)
    amps = lax.dot_general(
        amp_rows[...].astype(BF16), spread, (((0,), (0,)), ((), ())), preferred_element_type=F32)
    pair, at = iota((NV * NC, wide), 0), iota((NV * NC, wide), 1)
    amps = jnp.where((pair >> 2) == (at & 3), amps, 0.0).astype(BF16)
    lines, pairs = iota((TILE, NV * NC), 0), iota((TILE, NV * NC), 1)
    amps = jnp.dot(one_hot((lines & 3) == (pairs & 3)).astype(BF16), amps, preferred_element_type=F32)
    amps = jnp.where(same_band, amps, 0.0)
    val_load.wait()
    for k in range(local_k):
        val_k = val_in[k].reshape(wide, width)
        for chunk in range(wide // TILE):
            mix = jnp.where(hits[k, chunk], amps, 0.0).astype(BF16)
            stored(zeta_send, k, chunk, jnp.dot(mix, val_k, preferred_element_type=F32))
    inner = (z > 0) & (z < line - 1)

    @pl.when(inner)
    def _():
        sent(zeta_order, lambda shift: zeta_copy(shift).start())

    zeta_all[me] = zeta_send[me]

    across(me)
    received(near, lambda shift: across(from_blk(shift)))
    received(far_first, relay)

    @pl.when(jnp.logical_not(inner))
    def _():
        sent(zeta_order, lambda shift: zeta_copy(shift).start())


    block = local_k * ROWS
    half = blks // 2
    group = min(half, TILE // block)
    low = z < line // 2

    def gathered(which):
        awaited(con_all.at[pl.ds(0, rings), pl.ds(0, half)], core_rsem.at[which]).wait_recv()
        for part in range(half // group):
            first = which * half + part * group
            for label in range(labels):
                summed = None
                for quarter in range(gas):
                    cons = con_all[quarter, pl.ds(first, group), label].reshape(group * block, width)
                    term = jnp.dot(cons, w_in[label, pl.ds(quarter * width, width), :], preferred_element_type=F32)
                    summed = term if summed is None else summed + term
                unit[pl.ds(first, group), label] = summed.astype(BF16).reshape(group, block, width)

    far_half = jnp.where(low, 1, 0)
    received(far_first, lambda shift: across(from_blk(shift)))
    w_load.wait()
    gathered(1 - far_half)
    gathered(far_half)

    def fin_copy(to):
        return pltpu.make_async_remote_copy(
            src_ref=contrib.at[to // gas], dst_ref=fin.at[lane],
            send_sem=send_sem.at[5], recv_sem=fin_rsem,
            device_id=(to // gas, to % gas), device_id_type=MESH)

    def finish(first, count):
        for turn in range(count):
            owner = first + turn

            @pl.when(owner != me)
            def _():
                awaited(zeta_all.at[owner], zeta_rsem.at[owner]).wait_recv()
        rows = count * block
        r, s = iota((rows, rows), 0), iota((rows, rows), 1)
        kept = ((r >> 4) == (s >> 4)) & ((r & 3) == (s & 3))
        cross = None
        for label in range(labels):
            units = unit[pl.ds(first, count), label].reshape(rows, width)
            zetas = zeta_all[pl.ds(first, count), label].reshape(rows, width)
            term = lax.dot_general(units, zetas, (((1,), (1,)), ((), ())), preferred_element_type=F32)
            cross = term if cross is None else cross + term
        folded = jnp.sum(jnp.where(kept, cross, 0.0).reshape(rows // ROWS, ROWS, rows), axis=0)
        if rows < LANES:
            folded = jnp.concatenate([folded, jnp.zeros((ROWS, LANES - rows), F32)], axis=1)
        lanes = iota((ROWS, LANES), 1)
        for step in (1, 2):
            folded = folded + jnp.where(
                (lanes & step) == 0, pltpu.roll(folded, LANES - step, 1), pltpu.roll(folded, step, 1))
        mine = jnp.sum(jnp.where((iota((ROWS, LANES), 0) >> 2) == (lanes & 3), folded, 0.0), axis=0, keepdims=True)
        for turn in range(count):
            contrib[first + turn] = mine if turn == 0 else pltpu.roll(mine, LANES - turn * block, 1)
        for turn in range(count):
            for part in range(gas):
                to = (first + turn) * gas + part

                @pl.when(to != lane)
                def _():
                    fin_copy(to).start()

                @pl.when(to == lane)
                def _():
                    fin[lane] = contrib[me]

    wave = LANES // block
    for step in range(line // 2):
        if step == line // 2 - 1:
            for at in range(half // wave):
                finish((1 - far_half) * half + at * wave, wave)
        finish(2 * jnp.where(low, line - 1 - step, step), 2)

    awaited(amp_all.at[pl.ds(0, blks - 1)], send_sem.at[0]).wait_send()
    awaited(con_send.at[pl.ds(0, blks - 1)], send_sem.at[1]).wait_send()
    awaited(zeta_send.at[pl.ds(0, blks - 1)], send_sem.at[2]).wait_send()
    awaited(con_all.at[pl.ds(0, rings - 1)], send_sem.at[3]).wait_send()
    awaited(con_all.at[pl.ds(0, rings)], send_sem.at[4]).wait_send()
    awaited(fin.at[pl.ds(0, devices - 1)], send_sem.at[5]).wait_send()
    awaited(fin.at[pl.ds(0, devices - 1)], fin_rsem).wait_recv()
    total_row = jnp.sum(fin[...], axis=0) / total
    for k in range(local_k):
        out_ref[k : k + 1, :] = total_row[:, k * ROWS : (k + 1) * ROWS]


def body(pair_val, pair_con, screened, amplitude, qmap, *, blks, gas):
    local_k, total, _, width = pair_val.shape
    labels, depth, _ = screened.shape
    devices = blks * gas
    dma = pltpu.SemaphoreType.DMA
    anywhere = pl.BlockSpec(memory_space=pl.ANY)
    vmem = pl.BlockSpec(memory_space=pltpu.VMEM)
    block = (labels, local_k * ROWS, width)
    return pl.pallas_call(
        functools.partial(kernel, blks, gas),
        out_shape=pltpu.VMEM((local_k, NV * NC), F32),
        in_specs=[anywhere] * 5,
        out_specs=vmem,
        scratch_shapes=[
            pltpu.VMEM(qmap.shape, jnp.int32),
            pltpu.VMEM(amplitude.shape, BF16),
            pltpu.VMEM(pair_val.shape, BF16),
            pltpu.VMEM(pair_con.shape, BF16),
            pltpu.VMEM(screened.shape, BF16),
            pltpu.VMEM((blks,) + block, BF16),
            pltpu.VMEM((blks,) + block, BF16),
            pltpu.VMEM((gas, blks) + block, BF16),
            pltpu.VMEM((blks,) + block, BF16),
            pltpu.VMEM((blks,) + amplitude.shape, BF16),
            pltpu.VMEM((total, NV * NC), F32),
            pltpu.VMEM((blks,) + block, BF16),
            pltpu.VMEM((blks, 1, 128), F32),
            pltpu.VMEM((devices, 1, 128), F32),
            dma((4 + local_k,)),
            dma((6,)), dma, dma((blks,)), dma((blks,)), dma((gas // 2 - 1, blks)), dma((2,)), dma,
        ],
        compiler_params=pltpu.CompilerParams(
            collective_id=0, has_side_effects=True, vmem_limit_bytes=60 * 1024 * 1024),
    )(pair_val, pair_con, screened, amplitude, qmap)


def solution(mesh):
    placed = (
        P("blk", None, None, "ga"),
        P("blk", None, None, "ga"),
        P("blk", None, "ga"),
        P("blk", None),
        P("blk", None),
    )
    sizes = {"blks": mesh.shape["blk"], "gas": mesh.shape["ga"]}
    return jax.shard_map(
        functools.partial(body, **sizes), mesh=mesh, in_specs=placed, out_specs=P("blk", None), check_vma=False
    )
```

```python
import functools

import jax
import jax.numpy as jnp
from jax import lax
from jax.experimental import pallas as pl
from jax.experimental.pallas import tpu as pltpu
from jax.sharding import PartitionSpec as P

NV = 4
NC = 4
ROWS = 16
TILE = 256
LANES = 128
MESH = pl.DeviceIdType.MESH
F32 = jnp.float32
BF16 = jnp.bfloat16


def iota(shape, dim):
    return lax.broadcasted_iota(jnp.int32, shape, dim)


def one_hot(mask):
    return jnp.where(mask, 1.0, 0.0).astype(F32)


def kernel(
    blks, gas, val_hbm, con_hbm, w_hbm, amp_hbm, q_hbm, out_ref,
    q_in, amp_in, val_in, con_in, w_in, con_send, zeta_send, con_all, zeta_all, amp_all, amp_rows, unit, contrib, fin,
    load_sem, hop_sem, send_sem, amp_rsem, con_rsem, zeta_rsem, row_rsem, core_rsem, fin_rsem,
):
    me, ga = lax.axis_index("blk"), lax.axis_index("ga")
    local_k, total = q_in.shape
    labels, width = w_in.shape[0], w_in.shape[2]
    wide = total * ROWS
    lane = me * gas + ga
    devices = blks * gas
    rings = gas // 2
    other = ga + 1 - 2 * (ga % 2)
    line = blks // 2
    z, x = me // 2, me % 2
    beside = jnp.minimum(z, 1) + jnp.minimum(line - 1 - z, 1)
    barrier = pltpu.get_barrier_semaphore()

    def greet(semaphore):
        for far in (1, -1):
            @pl.when((z + far >= 0) & (z + far < line))
            def _():
                pl.semaphore_signal(semaphore, inc=1, device_id=(me + 2 * far, ga), device_id_type=MESH)

    greet(barrier)
    pl.semaphore_signal(barrier, inc=1, device_id=(z * 2 + (x + 1) % 2, ga), device_id_type=MESH)
    pl.semaphore_signal(barrier, inc=1, device_id=(me, other), device_id_type=MESH)
    for hop in range(1, rings):
        pl.semaphore_signal(barrier, inc=1, device_id=(me, (ga + 2 * hop) % gas), device_id_type=MESH)


    q_load = pltpu.make_async_copy(q_hbm, q_in, load_sem.at[0])
    amp_load = pltpu.make_async_copy(amp_hbm, amp_in, load_sem.at[1])
    val_load = pltpu.make_async_copy(val_hbm, val_in, load_sem.at[2])
    w_load = pltpu.make_async_copy(w_hbm, w_in, load_sem.at[3])
    con_loads = [pltpu.make_async_copy(con_hbm.at[k], con_in.at[k], load_sem.at[4 + k]) for k in range(local_k)]
    for load in [q_load, *con_loads, amp_load]:
        load.start()

    def both(*steps):
        return [(sign * far, turn) for far in steps for turn in (1, 0) for sign in (1, -1)]

    far_first = both(*range(line - 1, 1, -1))
    near = both(1) + [(0, 1)]
    con_order = near + far_first
    zeta_order = [(0, 1)] + far_first + both(1)

    def to_blk(shift):
        return (z + shift[0]) * 2 + (x + shift[1]) % 2

    def from_blk(shift):
        return (z - shift[0]) * 2 + (x + shift[1]) % 2

    def sent(chosen, action):
        for shift in chosen:
            pl.when((z + shift[0] >= 0) & (z + shift[0] < line))(functools.partial(action, shift))

    def received(chosen, action):
        for shift in chosen:
            pl.when((z - shift[0] >= 0) & (z - shift[0] < line))(functools.partial(action, shift))

    def blk_copy(src, dst, ssem, rsem, to):
        return pltpu.make_async_remote_copy(
            src_ref=src, dst_ref=dst, send_sem=ssem, recv_sem=rsem, device_id=(to, ga), device_id_type=MESH)

    def amp_copy(shift):
        return blk_copy(amp_in, amp_all.at[me], send_sem.at[0], amp_rsem, to_blk(shift))

    def con_copy(shift):
        to = to_blk(shift)
        return blk_copy(con_send.at[to], con_all.at[ga, me], send_sem.at[1], con_rsem.at[me], to)

    def zeta_copy(shift):
        to = to_blk(shift)
        return blk_copy(zeta_send.at[to], zeta_all.at[me], send_sem.at[2], zeta_rsem.at[me], to)

    def awaited(ref, sem):
        return pltpu.make_async_remote_copy(
            src_ref=ref, dst_ref=ref, send_sem=sem, recv_sem=sem, device_id=(me, other), device_id_type=MESH)

    def row_copy(hop, owner):
        return pltpu.make_async_remote_copy(
            src_ref=con_all.at[ga, owner], dst_ref=con_all.at[ga, owner],
            send_sem=send_sem.at[3], recv_sem=row_rsem.at[hop - 1, owner],
            device_id=(me, (ga + 2 * hop) % gas), device_id_type=MESH)

    def core_copy(hop, owner):
        part = (ga + gas - 2 * hop) % gas
        return pltpu.make_async_remote_copy(
            src_ref=con_all.at[part, owner], dst_ref=con_all.at[part, owner],
            send_sem=send_sem.at[4], recv_sem=core_rsem.at[owner // (blks // 2)],
            device_id=(me, other), device_id_type=MESH)

    def hand_on(owner):
        for hop in range(1, rings):
            row_copy(hop, owner).start()
        core_copy(0, owner).start()

    def across(owner):
        for hop in range(1, rings):
            row_copy(hop, owner).wait_recv()
            core_copy(hop, owner).start()

    half = blks // 2
    low = z < line // 2
    far_half = jnp.where(low, 1, 0)
    mine = [(1 - far_half) * half + at for at in range(half)]
    theirs = [2 * jnp.where(low, line - 1 - at // 2, at // 2) + at % 2 for at in range(half)]

    def others(owners, action):
        for owner in owners:
            pl.when(owner != me)(functools.partial(action, owner))

    def relay(owner):
        awaited(con_all.at[ga, owner], con_rsem.at[owner]).wait_recv()
        hand_on(owner)

    spread = one_hot(iota((total, wide), 1) >> 4 == iota((total, wide), 0)).astype(BF16)
    row, col = iota((TILE, wide), 0), iota((TILE, wide), 1)
    same_pair = (row & 15) == (col & 15)
    same_band = ((row >> 2) & 3) == ((col >> 2) & 3)
    chunk_labels = TILE // ROWS
    chunk_blks = chunk_labels // labels

    def stored(ref, k, chunk, value):
        blocks = value.astype(BF16).reshape(chunk_blks, labels, ROWS, width)
        ref[pl.ds(chunk * chunk_blks, chunk_blks), :, pl.ds(k * ROWS, ROWS), :] = blocks

    q_load.wait()
    labels_at = jnp.dot(q_in[...].astype(F32).astype(BF16), spread, preferred_element_type=F32).astype(jnp.int32)
    hits = {}
    for k in range(local_k):
        for chunk in range(wide // TILE):
            hits[k, chunk] = labels_at[k : k + 1, :] == (row >> 4) + chunk * chunk_labels
    for k in range(local_k):
        con_loads[k].wait()
        con_k = con_in[k].reshape(wide, width)
        for chunk in range(wide // TILE):
            pick = one_hot(hits[k, chunk] & same_pair).astype(BF16)
            stored(con_send, k, chunk, jnp.dot(pick, con_k, preferred_element_type=F32))
    amp_load.wait()
    val_load.start()
    w_load.start()

    pl.semaphore_wait(barrier, beside + rings + 1)
    inner = (z > 0) & (z < line - 1)
    turned = [shift for shift in con_order if shift[1] == 1 and shift[0] != 0]

    def straight(far):
        return [(far, 0), (-far, 0)] if far < line else []

    for phase in range(1, line + 1):
        if phase > 1:
            pl.semaphore_wait(hop_sem.at[phase - 2], beside)
        if phase < line:
            greet(hop_sem.at[phase - 1])
        reached = [shift for shift in con_order if abs(shift[0]) + shift[1] == phase]
        sent(reached, lambda shift: amp_copy(shift).start())
        if phase == 1:
            sent(reached, lambda shift: con_copy(shift).start())
        else:
            sent(straight(phase), lambda shift: pl.when(inner)(con_copy(shift).start))
        if phase == 2:
            sent([(1, 1), (-1, 1)], lambda shift: pl.when(jnp.logical_not(inner))(con_copy(shift).start))
        if phase == line - 1:
            sent(turned, lambda shift: pl.when(inner)(con_copy(shift).start))
        if phase == line:
            for far in range(line - 1, 1, -1):
                sent(straight(far), lambda shift: pl.when(jnp.logical_not(inner))(con_copy(shift).start))
            sent(turned[2:], lambda shift: pl.when(jnp.logical_not(inner))(con_copy(shift).start))
        if phase == 1:
            con_all[ga, me] = con_send[me]
            amp_all[me] = amp_in[...]
            hand_on(me)

    others(mine, relay)

    awaited(amp_all.at[pl.ds(0, blks - 1)], amp_rsem).wait_recv()
    for blk in range(blks):
        amp_rows[pl.ds(blk * local_k, local_k), :] = amp_all[blk].astype(F32)
    amps = lax.dot_general(
        amp_rows[...].astype(BF16), spread, (((0,), (0,)), ((), ())), preferred_element_type=F32)
    pair, at = iota((NV * NC, wide), 0), iota((NV * NC, wide), 1)
    amps = jnp.where((pair >> 2) == (at & 3), amps, 0.0).astype(BF16)
    lines, pairs = iota((TILE, NV * NC), 0), iota((TILE, NV * NC), 1)
    amps = jnp.dot(one_hot((lines & 3) == (pairs & 3)).astype(BF16), amps, preferred_element_type=F32)
    amps = jnp.where(same_band, amps, 0.0)
    val_load.wait()
    for k in range(local_k):
        val_k = val_in[k].reshape(wide, width)
        for chunk in range(wide // TILE):
            mix = jnp.where(hits[k, chunk], amps, 0.0).astype(BF16)
            stored(zeta_send, k, chunk, jnp.dot(mix, val_k, preferred_element_type=F32))
    def crosses(shift):
        return (z + shift[0] >= line // 2) == low

    def zeta_start(held, shift):
        pl.when(jnp.logical_not(inner | jnp.logical_not(crosses(shift))) == held)(zeta_copy(shift).start)

    sent(zeta_order, functools.partial(zeta_start, False))
    zeta_all[me] = zeta_send[me]

    across(me)
    others(mine, across)
    for owner in theirs:
        relay(owner)

    sent(zeta_order, functools.partial(zeta_start, True))

    block = local_k * ROWS
    group = min(half, TILE // block)

    def gathered(which):
        awaited(con_all.at[pl.ds(0, rings), pl.ds(0, half)], core_rsem.at[which]).wait_recv()
        for part in range(half // group):
            first = which * half + part * group
            for label in range(labels):
                summed = None
                for quarter in range(gas):
                    cons = con_all[quarter, pl.ds(first, group), label].reshape(group * block, width)
                    term = jnp.dot(cons, w_in[label, pl.ds(quarter * width, width), :], preferred_element_type=F32)
                    summed = term if summed is None else summed + term
                unit[pl.ds(first, group), label] = summed.astype(BF16).reshape(group, block, width)

    for owner in theirs:
        across(owner)
    w_load.wait()
    gathered(1 - far_half)
    gathered(far_half)

    def fin_copy(to):
        return pltpu.make_async_remote_copy(
            src_ref=contrib.at[to // gas], dst_ref=fin.at[lane],
            send_sem=send_sem.at[5], recv_sem=fin_rsem,
            device_id=(to // gas, to % gas), device_id_type=MESH)

    def finish(first, count):
        for turn in range(count):
            owner = first + turn

            @pl.when(owner != me)
            def _():
                awaited(zeta_all.at[owner], zeta_rsem.at[owner]).wait_recv()
        rows = count * block
        r, s = iota((rows, rows), 0), iota((rows, rows), 1)
        kept = ((r >> 4) == (s >> 4)) & ((r & 3) == (s & 3))
        cross = None
        for label in range(labels):
            units = unit[pl.ds(first, count), label].reshape(rows, width)
            zetas = zeta_all[pl.ds(first, count), label].reshape(rows, width)
            term = lax.dot_general(units, zetas, (((1,), (1,)), ((), ())), preferred_element_type=F32)
            cross = term if cross is None else cross + term
        folded = jnp.sum(jnp.where(kept, cross, 0.0).reshape(rows // ROWS, ROWS, rows), axis=0)
        if rows < LANES:
            folded = jnp.concatenate([folded, jnp.zeros((ROWS, LANES - rows), F32)], axis=1)
        lanes = iota((ROWS, LANES), 1)
        for step in (1, 2):
            folded = folded + jnp.where(
                (lanes & step) == 0, pltpu.roll(folded, LANES - step, 1), pltpu.roll(folded, step, 1))
        mine = jnp.sum(jnp.where((iota((ROWS, LANES), 0) >> 2) == (lanes & 3), folded, 0.0), axis=0, keepdims=True)
        for turn in range(count):
            contrib[first + turn] = mine if turn == 0 else pltpu.roll(mine, LANES - turn * block, 1)
        for turn in range(count):
            for part in range(gas):
                to = (first + turn) * gas + part

                @pl.when(to != lane)
                def _():
                    fin_copy(to).start()

                @pl.when(to == lane)
                def _():
                    fin[lane] = contrib[me]

    wave = LANES // block
    for step in range(line // 2):
        if step == line // 2 - 1:
            for at in range(half // wave):
                finish((1 - far_half) * half + at * wave, wave)
        finish(2 * jnp.where(low, line - 1 - step, step), 2)

    awaited(amp_all.at[pl.ds(0, blks - 1)], send_sem.at[0]).wait_send()
    awaited(con_send.at[pl.ds(0, blks - 1)], send_sem.at[1]).wait_send()
    awaited(zeta_send.at[pl.ds(0, blks - 1)], send_sem.at[2]).wait_send()
    awaited(con_all.at[pl.ds(0, rings - 1)], send_sem.at[3]).wait_send()
    awaited(con_all.at[pl.ds(0, rings)], send_sem.at[4]).wait_send()
    awaited(fin.at[pl.ds(0, devices - 1)], send_sem.at[5]).wait_send()
    awaited(fin.at[pl.ds(0, devices - 1)], fin_rsem).wait_recv()
    total_row = jnp.sum(fin[...], axis=0) / total
    for k in range(local_k):
        out_ref[k : k + 1, :] = total_row[:, k * ROWS : (k + 1) * ROWS]


def body(pair_val, pair_con, screened, amplitude, qmap, *, blks, gas):
    local_k, total, _, width = pair_val.shape
    labels, depth, _ = screened.shape
    devices = blks * gas
    dma = pltpu.SemaphoreType.DMA
    anywhere = pl.BlockSpec(memory_space=pl.ANY)
    vmem = pl.BlockSpec(memory_space=pltpu.VMEM)
    block = (labels, local_k * ROWS, width)
    return pl.pallas_call(
        functools.partial(kernel, blks, gas),
        out_shape=pltpu.VMEM((local_k, NV * NC), F32),
        in_specs=[anywhere] * 5,
        out_specs=vmem,
        scratch_shapes=[
            pltpu.VMEM(qmap.shape, jnp.int32),
            pltpu.VMEM(amplitude.shape, BF16),
            pltpu.VMEM(pair_val.shape, BF16),
            pltpu.VMEM(pair_con.shape, BF16),
            pltpu.VMEM(screened.shape, BF16),
            pltpu.VMEM((blks,) + block, BF16),
            pltpu.VMEM((blks,) + block, BF16),
            pltpu.VMEM((gas, blks) + block, BF16),
            pltpu.VMEM((blks,) + block, BF16),
            pltpu.VMEM((blks,) + amplitude.shape, BF16),
            pltpu.VMEM((total, NV * NC), F32),
            pltpu.VMEM((blks,) + block, BF16),
            pltpu.VMEM((blks, 1, 128), F32),
            pltpu.VMEM((devices, 1, 128), F32),
            dma((4 + local_k,)),
            pltpu.SemaphoreType.REGULAR((max(blks // 2 - 1, 1),)), dma((6,)), dma, dma((blks,)), dma((blks,)), dma((gas // 2 - 1, blks)), dma((2,)), dma,
        ],
        compiler_params=pltpu.CompilerParams(
            collective_id=0, has_side_effects=True, vmem_limit_bytes=60 * 1024 * 1024),
    )(pair_val, pair_con, screened, amplitude, qmap)


def solution(mesh):
    placed = (
        P("blk", None, None, "ga"),
        P("blk", None, None, "ga"),
        P("blk", None, "ga"),
        P("blk", None),
        P("blk", None),
    )
    sizes = {"blks": mesh.shape["blk"], "gas": mesh.shape["ga"]}
    return jax.shard_map(
        functools.partial(body, **sizes), mesh=mesh, in_specs=placed, out_specs=P("blk", None), check_vma=False
    )
```
